32 devices in a mesh: rep: 2 (over x), dp: 16 (over y, z, core).
Axes of the slice: x: 2, y: 2, z: 4, core: 2. Of those that a mesh axis runs over, the one named last changes fastest.
Arguments:
- x: bfloat16 [32, 2048, 768], P(('rep', 'dp')), parts along dimension 0
- dy: bfloat16 [32, 2048, 768], P(('rep', 'dp')), parts along dimension 0
- wq: bfloat16 [2, 768, 768], replicated
- wk: bfloat16 [2, 768, 128], replicated
- wv: bfloat16 [2, 768, 128], replicated
- wo: bfloat16 [2, 768, 768], replicated
- w_gate: bfloat16 [2, 768, 2048], replicated
- w_up: bfloat16 [2, 768, 2048], replicated
- w_down: bfloat16 [2, 2048, 768], replicated
- m_wq: float32 [2, 768, 768], P(None, 'dp')
- m_wk: float32 [2, 768, 128], P(None, 'dp')
- m_wv: float32 [2, 768, 128], P(None, 'dp')
- m_wo: float32 [2, 768, 768], P(None, 'dp')
- m_w_gate: float32 [2, 768, 2048], P(None, 'dp')
- m_w_up: float32 [2, 768, 2048], P(None, 'dp')
- m_w_down: float32 [2, 2048, 768], P(None, 'dp')
- v_wq: float32 [2, 768, 768], P(None, 'dp')
- v_wk: float32 [2, 768, 128], P(None, 'dp')
- v_wv: float32 [2, 768, 128], P(None, 'dp')
- v_wo: float32 [2, 768, 768], P(None, 'dp')
- v_w_gate: float32 [2, 768, 2048], P(None, 'dp')
- v_w_up: float32 [2, 768, 2048], P(None, 'dp')
- v_w_down: float32 [2, 2048, 768], P(None, 'dp')
Outputs:
- output 1: bfloat16 [4, 768, 768], P('rep'), parts along dimension 0
- output 2: bfloat16 [4, 768, 128], P('rep'), parts along dimension 0
- output 3: bfloat16 [4, 768, 128], P('rep'), parts along dimension 0
- output 4: bfloat16 [4, 768, 768], P('rep'), parts along dimension 0
- output 5: bfloat16 [4, 768, 2048], P('rep'), parts along dimension 0
- output 6: bfloat16 [4, 768, 2048], P('rep'), parts along dimension 0
- output 7: bfloat16 [4, 2048, 768], P('rep'), parts along dimension 0
- output 8: float32 [4, 768, 768], P('rep', 'dp'), parts along dimension 0
- output 9: float32 [4, 768, 128], P('rep', 'dp'), parts along dimension 0
- output 10: float32 [4, 768, 128], P('rep', 'dp'), parts along dimension 0
- output 11: float32 [4, 768, 768], P('rep', 'dp'), parts along dimension 0
- output 12: float32 [4, 768, 2048], P('rep', 'dp'), parts along dimension 0
- output 13: float32 [4, 768, 2048], P('rep', 'dp'), parts along dimension 0
- output 14: float32 [4, 2048, 768], P('rep', 'dp'), parts along dimension 0
- output 15: float32 [4, 768, 768], P('rep', 'dp'), parts along dimension 0
- output 16: float32 [4, 768, 128], P('rep', 'dp'), parts along dimension 0
- output 17: float32 [4, 768, 128], P('rep', 'dp'), parts along dimension 0
- output 18: float32 [4, 768, 768], P('rep', 'dp'), parts along dimension 0
- output 19: float32 [4, 768, 2048], P('rep', 'dp'), parts along dimension 0
- output 20: float32 [4, 768, 2048], P('rep', 'dp'), parts along dimension 0
- output 21: float32 [4, 2048, 768], P('rep', 'dp'), parts along dimension 0
There are 2 independent parts. The reference program is written for one: setup_inputs(seed, part) draws one part's arguments, and reference() takes and returns one part's arrays. A program takes and returns all parts, laid end to end along the dimension named above; an argument that names none is the same for every part.
All inputs are finite; a program needn't handle non-finite values.
Results may differ from the reference program's by a relative error of at most 0.024.
Values are sent between devices in bfloat16 or wider.
A program may use at most 2 GiB of HBM per device.

```python
import jax
import jax.numpy as jnp
from jax import lax

SEQUENCES = 16
TOKENS = 2048
D = 768
HEADS = 6
KV_HEADS = 1
HEAD = 128
FF = 2048
LAYERS = 2
THETA = 10000
NAMES = ("wq", "wk", "wv", "wo", "w_gate", "w_up", "w_down")
SHAPES = {
    "wq": (LAYERS, D, HEADS * HEAD),
    "wk": (LAYERS, D, KV_HEADS * HEAD),
    "wv": (LAYERS, D, KV_HEADS * HEAD),
    "wo": (LAYERS, HEADS * HEAD, D),
    "w_gate": (LAYERS, D, FF),
    "w_up": (LAYERS, D, FF),
    "w_down": (LAYERS, FF, D),
}


def bump(key, n, height):
    away = (jnp.arange(n, dtype=jnp.int32) - jax.random.randint(key, (), 0, n, jnp.int32)) % n
    return jnp.where(away < n // 8, height, 1.0)


def together(key, own, strength):
    shared = jax.random.normal(key, own.shape[1:], jnp.float32)
    return (own + strength * shared) * lax.rsqrt(1 + strength * strength)


def setup_inputs(seed: int = 0, part: int = 0) -> dict:
    kx, kdy, ka, kb, kz, kf, kh, kl, *keys = jax.random.split(jax.random.key(seed), 8 + 3 * len(NAMES))
    kx, kdy, ka, kb = (jax.random.fold_in(k, part) for k in (kx, kdy, ka, kb))
    kw, km, kv = (keys[i::3] for i in range(3))
    shape = (SEQUENCES, TOKENS, D)
    much_x, much_dy = jax.random.uniform(kz, (2,), jnp.float32, 0.0, 1.0)
    loud = 2.0 ** jax.random.uniform(jax.random.fold_in(kz, 1), (), jnp.float32, -1.0, 2.0)
    layers = 2.0 ** jax.random.uniform(kl, (LAYERS, 1, 1), jnp.float32, -1.0, 1.0)
    times = {"wq": 1.0, "wk": 1.0, "wv": 2.0, "wo": layers, "w_gate": 1.0, "w_up": bump(kh, FF, 4.0), "w_down": layers}
    x = together(ka, jax.random.normal(kx, shape, jnp.float32), much_x) * bump(kf, D, 4.0)
    dy = together(kb, jax.random.normal(kdy, shape, jnp.float32), much_dy)
    drawn = {"x": x.astype(jnp.bfloat16), "dy": (loud * dy * (SEQUENCES * TOKENS) ** -0.5).astype(jnp.bfloat16)}
    for key, name in zip(kw, NAMES, strict=True):
        drawn[name] = (jax.random.normal(key, SHAPES[name], jnp.float32) * SHAPES[name][1] ** -0.5 * times[name]).astype(jnp.bfloat16)
    for key, name in zip(km, NAMES, strict=True):
        drawn[f"m_{name}"] = 0.1 * jax.random.normal(key, SHAPES[name], jnp.float32)
    for key, name in zip(kv, NAMES, strict=True):
        drawn[f"v_{name}"] = jax.random.uniform(key, SHAPES[name], jnp.float32, 0.02, 0.06)
    return drawn


def matmul(a, w):
    return jnp.dot(a, w, preferred_element_type=jnp.float32).astype(jnp.bfloat16)


def normed(h):
    wide = h.astype(jnp.float32)
    scale = lax.rsqrt(jnp.mean(wide**2, -1, keepdims=True) + 1e-6)
    return (wide * scale).astype(jnp.bfloat16)


def turned(t, theta):
    half = t.shape[-1] // 2
    angle = jnp.arange(t.shape[0], dtype=jnp.float32)[:, None] * theta ** (-jnp.arange(half, dtype=jnp.float32) / half)
    cos, sin = jnp.cos(angle)[:, None], jnp.sin(angle)[:, None]
    a, b = t[..., :half].astype(jnp.float32), t[..., half:].astype(jnp.float32)
    return jnp.concatenate([a * cos - b * sin, b * cos + a * sin], -1).astype(jnp.bfloat16)


def seen_by(q, k, v):
    tokens, kv = q.shape[0], k.shape[1]
    q = q.reshape(tokens, kv, -1, q.shape[-1])
    scores = jnp.einsum("tgsd,ugd->gstu", q.astype(jnp.float32), k.astype(jnp.float32)) * q.shape[-1] ** -0.5
    place = jnp.arange(tokens)
    weights = jax.nn.softmax(jnp.where(place[:, None] >= place, scores, -jnp.inf), -1).astype(jnp.bfloat16)
    return jnp.einsum("gstu,ugd->tgsd", weights.astype(jnp.float32), v.astype(jnp.float32)).astype(jnp.bfloat16).reshape(tokens, -1)


def layer(h, w):
    a = normed(h)
    q, k = (turned(matmul(a, w[name]).reshape(h.shape[0], -1, HEAD), THETA) for name in ("wq", "wk"))
    h = h + matmul(seen_by(q, k, matmul(a, w["wv"]).reshape(h.shape[0], -1, HEAD)), w["wo"])
    b = normed(h)
    gate = jnp.dot(b, w["w_gate"], preferred_element_type=jnp.float32)
    up = jnp.dot(b, w["w_up"], preferred_element_type=jnp.float32)
    return h + matmul((jax.nn.silu(gate) * up).astype(jnp.bfloat16), w["w_down"])


def adamw(w, m, v, g):
    m = 0.9 * m + 0.1 * g
    v = 0.95 * v + 0.05 * g * g
    step = m * lax.rsqrt(v + 1e-8) + 0.1 * w
    return (w - 0.02 * step).astype(jnp.bfloat16), m, v


def clipped(gradients, sum_of_squares, count):
    factor = jnp.minimum(1.0, 0.5 * lax.rsqrt(sum_of_squares / count + 1e-30))
    return [g * factor for g in gradients]


def stack(weights, h):
    return lax.scan(lambda h, w: (layer(h, w), None), h, weights)[0]


def reference(x, dy, wq, wk, wv, wo, w_gate, w_up, w_down, m_wq, m_wk, m_wv, m_wo, m_w_gate, m_w_up, m_w_down, v_wq, v_wk, v_wv, v_wo, v_w_gate, v_w_up, v_w_down):
    weights = dict(zip(NAMES, (wq, wk, wv, wo, w_gate, w_up, w_down), strict=True))

    def take(so_far, sequence):
        h, by_y = sequence
        _, back = jax.vjp(stack, weights, h)
        by_weights, by_h = back(by_y)
        return jax.tree.map(lambda total, term: total + term.astype(jnp.float32), so_far, by_weights), by_h

    none_yet = {name: jnp.zeros(w.shape, jnp.float32) for name, w in weights.items()}
    by_weights, by_x = lax.scan(take, none_yet, (x, dy))
    gradients = [by_weights[name].astype(jnp.bfloat16).astype(jnp.float32) for name in NAMES]
    gradients = clipped(gradients, sum(jnp.sum(g * g) for g in gradients), sum(g.size for g in gradients))
    first = (m_wq, m_wk, m_wv, m_wo, m_w_gate, m_w_up, m_w_down)
    second = (v_wq, v_wk, v_wv, v_wo, v_w_gate, v_w_up, v_w_down)
    new = [adamw(weights[name].astype(jnp.float32), m, v, g) for name, m, v, g in zip(NAMES, first, second, gradients, strict=True)]
    return tuple(one[which] for which in range(3) for one in new)
```

```python
import functools

import jax
import jax.numpy as jnp
from jax import lax
from jax.experimental import pallas as pl
from jax.experimental.pallas import tpu as pltpu
from jax.sharding import PartitionSpec as P

NEG = -1e30
HIDDEN = 2 * NEG
LOG2E = 1.4426950408889634
VMEM = 62 * 2**20
HEAD = 128
THETA = 10000
EPS = 1e-6
F32, BF16 = jnp.float32, jnp.bfloat16


def _dot(a, b, ca, cb):
    return lax.dot_general(a, b, (((ca,), (cb,)), ((), ())), preferred_element_type=F32)


def _params(*semantics):
    return pltpu.CompilerParams(dimension_semantics=semantics, vmem_limit_bytes=VMEM)


def _cost(flops, arrays, exps=0):
    return pl.CostEstimate(flops=int(flops), transcendentals=int(exps), bytes_accessed=sum(a.size * a.dtype.itemsize for a in arrays))


def _rows(n):
    return slice(n * HEAD, (n + 1) * HEAD)


def _scale(wide):
    return lax.rsqrt(jnp.mean(wide * wide, -1, keepdims=True) + EPS)


def _normed(h):
    wide = h.astype(F32)
    return (wide * _scale(wide)).astype(BF16)


def _norm_bwd(h, ct):
    wide, c = h.astype(F32), ct.astype(BF16).astype(F32)
    scale = _scale(wide)
    back = jnp.mean(c * wide, -1, keepdims=True) * (scale * scale * scale)
    return (c * scale - wide * back).astype(BF16)


def _turn(t, cos, sin):
    t = t.astype(F32)
    return (t * cos + pltpu.roll(t, HEAD // 2, 1) * sin).astype(BF16)


def _turn_back(t, cos, sin):
    t = t.astype(F32)
    return (t * cos - pltpu.roll(t, HEAD // 2, 1) * sin).astype(BF16)


def _whole(shape, layer=None):
    if layer is None:
        return pl.BlockSpec(shape, lambda *_: (0,) * len(shape), pipeline_mode=pl.Buffered(1))
    return pl.BlockSpec((1, *shape), lambda *_: (layer,) + (0,) * len(shape), pipeline_mode=pl.Buffered(1))


def _pack(ref, at, value, height):
    for c in range(value.shape[1] // 256):
        piece = value[:, c * 256 : (c + 1) * 256].astype(BF16)
        ref[:, at + c * height : at + (c + 1) * height, :] = piece.reshape(-1, height, 256)


def _project(h_ref, wq_ref, wk_ref, wv_ref, cos_ref, sin_ref, q_ref, k_ref, v_ref):
    a = _normed(h_ref[...])
    cos, sin = cos_ref[...], sin_ref[...]
    q = _dot(a, wq_ref[0], 1, 0).astype(BF16)
    for n in range(q.shape[1] // HEAD):
        q_ref[:, _rows(n)] = _turn(q[:, _rows(n)], cos, sin)
    k_ref[...] = _turn(_dot(a, wk_ref[0], 1, 0).astype(BF16), cos, sin)
    v_ref[...] = _dot(a, wv_ref[0], 1, 0).astype(BF16)


def project(h, wq, wk, wv, cos, sin, layer, bt=512):
    t, d = h.shape
    tokens = lambda width: pl.BlockSpec((bt, width), lambda i: (i, 0))
    wide, one = wq.shape[2], wk.shape[2]
    outs = [jax.ShapeDtypeStruct((t, w), BF16) for w in (wide, one, one)]
    return pl.pallas_call(
        _project,
        grid=(t // bt,),
        in_specs=[tokens(d), _whole((d, wide), layer), _whole((d, one), layer), _whole((d, one), layer), tokens(HEAD), tokens(HEAD)],
        out_specs=[tokens(wide), tokens(one), tokens(one)],
        out_shape=outs,
        compiler_params=_params("arbitrary"),
        cost_estimate=_cost(2 * t * d * (wide + 2 * one), [h, cos, sin, *outs]),
        name="project",
    )(h, wq, wk, wv, cos, sin)


def _attend(q_ref, k_ref, v_ref, o_ref, lse_ref, top_s, mix_s, gap_s, *, heads, bq, bk, scale):
    iq = pl.program_id(0)
    e = scale * LOG2E
    cols = [slice(n * bq, (n + 1) * bq) for n in range(heads)]

    @pl.when(iq == 0)
    def _():
        gap_s[...] = lax.broadcasted_iota(jnp.int32, (bk, bq), 1) - lax.broadcasted_iota(jnp.int32, (bk, bq), 0)

    top_s[...] = jnp.full(top_s.shape, NEG, F32)
    mix_s[...] = jnp.zeros(mix_s.shape, F32)
    ones = jnp.ones((8, bk), BF16)

    def block(j, masked):
        here = pl.ds(pl.multiple_of(j * bk, bk), bk)
        key = k_ref[here, :]
        scores = [_dot(key, q_ref[:, _rows(n)], 1, 1) for n in range(heads)]
        ok = gap_s[...] >= j * bk - iq * bq if masked else None
        weights, keeps = [], []
        for n, s in enumerate(scores):
            if masked:
                s = jnp.where(ok, s, HIDDEN)
            old = top_s[:, cols[n]]
            top = jnp.maximum(old, s.max(axis=0, keepdims=True))
            top_s[:, cols[n]] = top
            weights.append(jnp.exp2((s - top) * e).astype(BF16))
            keeps.append(jnp.exp2((old - top) * e))
        values = jnp.concatenate([v_ref[here, :].T, ones], axis=0)
        for n, (p, keep) in enumerate(zip(weights, keeps)):
            mix_s[:, cols[n]] = mix_s[:, cols[n]] * keep + _dot(values, p, 1, 0)

    whole = lax.div(iq * bq, bk)
    lax.fori_loop(0, whole, lambda j, _: block(j, False), None)
    lax.fori_loop(whole, lax.div(iq * bq + bq, bk), lambda j, _: block(j, True), None)
    for n in range(heads):
        total = mix_s[HEAD : HEAD + 1, cols[n]]
        o_ref[:, _rows(n)] = (mix_s[:HEAD, cols[n]] * (1 / total)).T.astype(BF16)
        lse_ref[n : n + 1, :] = top_s[:, cols[n]] * scale + jnp.log(total)


def attend(q, k, v, bq=512, bk=512):
    t, wide = q.shape
    heads = wide // HEAD
    outs = [jax.ShapeDtypeStruct((t, wide), BF16), jax.ShapeDtypeStruct((heads, t), F32)]
    return pl.pallas_call(
        functools.partial(_attend, heads=heads, bq=bq, bk=bk, scale=HEAD**-0.5),
        grid=(t // bq,),
        in_specs=[pl.BlockSpec((bq, wide), lambda i: (i, 0)), _whole((t, HEAD)), _whole((t, HEAD))],
        out_specs=[pl.BlockSpec((bq, wide), lambda i: (i, 0)), pl.BlockSpec((heads, bq), lambda i: (0, i))],
        out_shape=outs,
        scratch_shapes=[pltpu.VMEM((1, heads * bq), F32), pltpu.VMEM((HEAD + 8, heads * bq), F32), pltpu.VMEM((bk, bq), jnp.int32)],
        compiler_params=_params("arbitrary"),
        cost_estimate=_cost(4 * t * t * wide, [q, k, v, *outs], heads * t * t),
        name="attend",
    )(q, k, v)


def _feed(o_ref, h_ref, wo_ref, wg_ref, wu_ref, wd_ref, mid_ref, out_ref, *, bf):
    mid = h_ref[...] + _dot(o_ref[...], wo_ref[0], 1, 0).astype(BF16)
    mid_ref[...] = mid
    b = _normed(mid)
    total = None
    for at in range(0, wg_ref.shape[2], bf):
        gate = _dot(b, wg_ref[0, :, at : at + bf], 1, 0)
        up = _dot(b, wu_ref[0, :, at : at + bf], 1, 0)
        act = (gate * jax.nn.sigmoid(gate) * up).astype(BF16)
        term = _dot(act, wd_ref[0, at : at + bf, :], 1, 0)
        total = term if total is None else total + term
    out_ref[...] = mid + total.astype(BF16)


def feed(o, h, wo, wg, wu, wd, layer, bt=512, bf=512):
    t, d = h.shape
    ff = wg.shape[2]
    tokens = lambda width: pl.BlockSpec((bt, width), lambda i: (i, 0))
    outs = [jax.ShapeDtypeStruct((t, d), BF16)] * 2
    return pl.pallas_call(
        functools.partial(_feed, bf=bf),
        grid=(t // bt,),
        in_specs=[tokens(o.shape[1]), tokens(d), _whole(wo.shape[1:], layer), _whole((d, ff), layer), _whole((d, ff), layer), _whole((ff, d), layer)],
        out_specs=[tokens(d), tokens(d)],
        out_shape=outs,
        compiler_params=_params("arbitrary"),
        cost_estimate=_cost(2 * t * d * (o.shape[1] + 3 * ff), [o, h, *outs], t * ff),
        name="feed",
    )(o, h, wo, wg, wu, wd)


def _feed_bwd(mid_ref, dy_ref, wg_ref, wu_ref, wd_ref, *rest, bt, own, down, ff):
    pack_ref, dmid_ref, b_s, bt_s, dyt_s, db_s, dg_s, act_s = rest[-8:]
    j = pl.program_id(0)
    t, bf = mid_ref.shape[0], wg_ref.shape[2]
    blocks = [slice(at, at + bt) for at in range(0, t, bt)]

    @pl.when(j == 0)
    def _():
        for at in blocks:
            b = _normed(mid_ref[at, :])
            b_s[at, :] = b
            bt_s[:, at] = b.T
            dyt_s[:, at] = dy_ref[at, :].T
            db_s[at, :] = jnp.zeros((bt, db_s.shape[1]), F32)

    w_gate, w_up, w_down = wg_ref[0], wu_ref[0], wd_ref[0]
    both = jnp.concatenate([w_gate, w_up], axis=1)
    for at in blocks:
        b = b_s[at, :]
        gate = _dot(b, w_gate, 1, 0)
        up = _dot(b, w_up, 1, 0)
        dact = _dot(dy_ref[at, :], w_down, 1, 1).astype(BF16).astype(F32)
        s = jax.nn.sigmoid(gate)
        silu = gate * s
        act_s[at, :] = (silu * up).astype(BF16)
        dup = (dact * silu).astype(BF16)
        dgate = (dact * up * (s + silu * (1 - s))).astype(BF16)
        dg_s[at, :bf] = dgate
        dg_s[at, bf:] = dup
        db_s[at, :] += _dot(dg_s[at, :], both, 1, 1)
    by_in = _dot(bt_s[...], dg_s[...], 1, 0)
    n = ff // 256
    for half in range(2):
        for c in range(bf // 256):
            piece = by_in[:, half * bf + c * 256 : half * bf + (c + 1) * 256].astype(BF16).reshape(-1, own, 256)
            at = pl.multiple_of((half * n + j * (bf // 256) + c) * own, own)
            pack_ref[:, pl.ds(at, own), :] = piece
    by_down = _dot(dyt_s[...], act_s[...], 1, 0).T.astype(BF16)
    for i in range(bf // down):
        for c in range(by_down.shape[1] // 256):
            at = 2 * n * own + c * down
            pack_ref[j * (bf // down) + i, at : at + down, :] = by_down[i * down : (i + 1) * down, c * 256 : (c + 1) * 256]

    @pl.when(j == pl.num_programs(0) - 1)
    def _():
        for at in blocks:
            dmid_ref[at, :] = dy_ref[at, :] + _norm_bwd(mid_ref[at, :], db_s[at, :])


def feed_bwd(mid, dy, wg, wu, wd, layer, group, packed=None, bt=512, bf=256):
    t, d = mid.shape
    ff = wg.shape[2]
    own, down = d // group, ff // group
    rows = (2 * own * ff + down * d) // 256
    height = rows if packed is None else packed.shape[1]
    more = [] if packed is None else [packed]
    outs = [jax.ShapeDtypeStruct((group, height, 256), BF16), jax.ShapeDtypeStruct((t, d), BF16)]
    return pl.pallas_call(
        functools.partial(_feed_bwd, bt=bt, own=own, down=down, ff=ff),
        grid=(ff // bf,),
        in_specs=[_whole((t, d)), _whole((t, d)), pl.BlockSpec((1, d, bf), lambda j: (layer, 0, j)), pl.BlockSpec((1, d, bf), lambda j: (layer, 0, j)),
                  pl.BlockSpec((1, bf, d), lambda j: (layer, j, 0))] + [pl.BlockSpec(memory_space=pl.ANY)] * len(more),
        input_output_aliases={5: 0} if more else {},
        out_specs=[_whole((group, rows, 256)), _whole((t, d))],
        out_shape=outs,
        scratch_shapes=[pltpu.VMEM((t, d), BF16), pltpu.VMEM((d, t), BF16), pltpu.VMEM((d, t), BF16), pltpu.VMEM((t, d), F32),
                        pltpu.VMEM((t, 2 * bf), BF16), pltpu.VMEM((t, bf), BF16)],
        compiler_params=_params("arbitrary"),
        cost_estimate=_cost(16 * t * d * ff, [mid, dy, *outs], t * ff),
        name="feed_bwd",
    )(mid, dy, wg, wu, wd, *more)


def _out_bwd(dmid_ref, o_ref, wo_ref, do_ref, delta_ref):
    do = _dot(dmid_ref[...], wo_ref[0], 1, 1).astype(BF16)
    do_ref[...] = do
    for n in range(do.shape[1] // HEAD):
        prod = do[:, _rows(n)].astype(F32) * o_ref[:, _rows(n)].astype(F32)
        delta_ref[n : n + 1, :] = prod.T.sum(axis=0, keepdims=True)


def out_bwd(dmid, o, wo, layer, bt=512):
    t, d = dmid.shape
    wide = o.shape[1]
    outs = [jax.ShapeDtypeStruct((t, wide), BF16), jax.ShapeDtypeStruct((wide // HEAD, t), F32)]
    tokens = lambda width: pl.BlockSpec((bt, width), lambda i: (i, 0))
    return pl.pallas_call(
        _out_bwd,
        grid=(t // bt,),
        in_specs=[tokens(d), tokens(wide), _whole((wide, d), layer)],
        out_specs=[tokens(wide), pl.BlockSpec((wide // HEAD, bt), lambda i: (0, i))],
        out_shape=outs,
        compiler_params=_params("arbitrary"),
        cost_estimate=_cost(2 * t * d * wide, [dmid, o, *outs]),
        name="out_bwd",
    )(dmid, o, wo)


def _attend_bwd(q_ref, k_ref, v_ref, do_ref, lse_ref, delta_ref, dq_ref, dk_ref, dv_ref, dq_s, dk_s, dv_s, gap_s, *, heads, bq, bk, pair, scale):
    iq = pl.program_id(0)
    e = scale * LOG2E
    wide = pair * bq
    groups = [range(n, n + pair) for n in range(0, heads, pair)]

    @pl.when(iq == 0)
    def _():
        gap_s[...] = lax.rem(lax.broadcasted_iota(jnp.int32, (bk, wide), 1), bq) - lax.broadcasted_iota(jnp.int32, (bk, wide), 0)
        dk_s[...] = jnp.zeros_like(dk_s)
        dv_s[...] = jnp.zeros_like(dv_s)

    dq_s[...] = jnp.zeros_like(dq_s)

    def block(j, masked):
        here = pl.ds(pl.multiple_of(j * bk, bk), bk)
        key, value = k_ref[here, :], v_ref[here, :]
        qs = [jnp.concatenate([q_ref[:, _rows(n)] for n in g], axis=0) for g in groups]
        dos = [jnp.concatenate([do_ref[:, _rows(n)] for n in g], axis=0) for g in groups]
        scores = [_dot(key, x, 1, 1) for x in qs]
        dps = [_dot(value, x, 1, 1) for x in dos]
        ok = gap_s[...] >= j * bk - iq * bq if masked else None
        for i, g in enumerate(groups):
            lse = jnp.concatenate([lse_ref[n : n + 1, :] for n in g], axis=1) * LOG2E
            delta = jnp.concatenate([delta_ref[n : n + 1, :] for n in g], axis=1)
            p = jnp.exp2(scores[i] * e - lse)
            if masked:
                p = jnp.where(ok, p, 0.0)
            ds = (p * (dps[i] - delta)).astype(BF16)
            dv_s[here, :] += _dot(p.astype(BF16), dos[i], 1, 0)
            dk_s[here, :] += _dot(ds, qs[i], 1, 0)
            dq_s[:, i * wide : (i + 1) * wide] += _dot(key.T, ds, 1, 0)

    whole = lax.div(iq * bq, bk)
    lax.fori_loop(0, whole, lambda j, _: block(j, False), None)
    lax.fori_loop(whole, lax.div(iq * bq + bq + bk - 1, bk), lambda j, _: block(j, True), None)
    for n in range(heads):
        dq_ref[:, _rows(n)] = (dq_s[:, n * bq : (n + 1) * bq] * scale).T.astype(BF16)

    @pl.when(iq == pl.num_programs(0) - 1)
    def _():
        dk_ref[...] = (dk_s[...] * scale).astype(BF16)
        dv_ref[...] = dv_s[...].astype(BF16)


def attend_bwd(q, k, v, do, lse, delta, bq=256, bk=512, pair=2):
    t, wide = q.shape
    heads = wide // HEAD
    outs = [jax.ShapeDtypeStruct((t, wide), BF16)] + [jax.ShapeDtypeStruct((t, HEAD), BF16)] * 2
    queries, stats = pl.BlockSpec((bq, wide), lambda i: (i, 0)), pl.BlockSpec((heads, bq), lambda i: (0, i))
    return pl.pallas_call(
        functools.partial(_attend_bwd, heads=heads, bq=bq, bk=bk, pair=pair, scale=HEAD**-0.5),
        grid=(t // bq,),
        in_specs=[queries, _whole((t, HEAD)), _whole((t, HEAD)), queries, stats, stats],
        out_specs=[queries, _whole((t, HEAD)), _whole((t, HEAD))],
        out_shape=outs,
        scratch_shapes=[pltpu.VMEM((HEAD, heads * bq), F32), pltpu.VMEM((t, HEAD), F32), pltpu.VMEM((t, HEAD), F32),
                        pltpu.VMEM((bk, pair * bq), jnp.int32)],
        compiler_params=_params("arbitrary"),
        cost_estimate=_cost(10 * t * t * wide, [q, k, v, do, *outs], heads * t * t),
        name="attend_bwd",
    )(q, k, v, do, lse, delta)


def _project_bwd(dq_ref, dk_ref, dv_ref, h_ref, dmid_ref, o_ref, wq_ref, wk_ref, wv_ref, cos_ref, sin_ref, pack_ref, dh_ref, qkv_s, o_s, *, own):
    i = pl.program_id(0)
    cos, sin = cos_ref[...], sin_ref[...]
    wide = dq_ref.shape[1]
    dq = jnp.concatenate([_turn_back(dq_ref[:, _rows(n)], cos, sin) for n in range(wide // HEAD)], axis=1)
    dkv = jnp.concatenate([_turn_back(dk_ref[...], cos, sin), dv_ref[...]], axis=1)
    h, dmid = h_ref[...], dmid_ref[...]
    by_a = _dot(dq, wq_ref[0], 1, 1) + _dot(dkv, jnp.concatenate([wk_ref[0], wv_ref[0]], axis=1), 1, 1)
    dh_ref[...] = dmid + _norm_bwd(h, by_a)
    a = _normed(h).T
    by_q, by_kv, by_o = _dot(a, dq, 1, 0), _dot(a, dkv, 1, 0), _dot(o_ref[...].T, dmid, 1, 0)

    @pl.when(i == 0)
    def _():
        qkv_s[:, :wide] = by_q
        qkv_s[:, wide:] = by_kv
        o_s[...] = by_o

    @pl.when(i > 0)
    def _():
        qkv_s[:, :wide] += by_q
        qkv_s[:, wide:] += by_kv
        o_s[...] += by_o

    @pl.when(i == pl.num_programs(0) - 1)
    def _():
        _pack(pack_ref, 0, qkv_s[...], own)
        used = qkv_s.shape[1] // 256 * own
        high = o_s.shape[0] // pack_ref.shape[0]
        _pack(pack_ref, used, o_s[...], high)
        used += o_s.shape[1] // 256 * high
        if used < pack_ref.shape[1]:
            pack_ref[:, used:, :] = jnp.zeros((pack_ref.shape[0], pack_ref.shape[1] - used, 256), BF16)


def project_bwd(dq, dk, dv, h, dmid, o, wq, wk, wv, cos, sin, layer, group, at, pack, bt=512):
    t, d = h.shape
    wide, one = dq.shape[1], dk.shape[1]
    rows = pack - at
    tokens = lambda width: pl.BlockSpec((bt, width), lambda i: (i, 0))
    outs = [jax.ShapeDtypeStruct((group, pack, 256), BF16), jax.ShapeDtypeStruct((t, d), BF16)]
    return pl.pallas_call(
        functools.partial(_project_bwd, own=d // group),
        grid=(t // bt,),
        in_specs=[tokens(wide), tokens(one), tokens(one), tokens(d), tokens(d), tokens(wide), _whole((d, wide), layer), _whole((d, one), layer),
                  _whole((d, one), layer), tokens(HEAD), tokens(HEAD)],
        out_specs=[pl.BlockSpec((group, rows, 256), lambda i: (0, at // rows, 0)), tokens(d)],
        out_shape=outs,
        scratch_shapes=[pltpu.VMEM((d, wide + 2 * one), F32), pltpu.VMEM((wide, d), F32)],
        compiler_params=_params("arbitrary"),
        cost_estimate=_cost(4 * t * d * (2 * wide + 2 * one), [dq, h, dmid, o, outs[1]]),
        name="project_bwd",
    )(dq, dk, dv, h, dmid, o, wq, wk, wv, cos, sin)


def _adamw(me_ref, factor_ref, *refs, places, unit):
    n = len(places)
    w, m, v = refs[:n], refs[n : 2 * n], refs[2 * n : 3 * n]
    (early, both, late), (fresh, *rest) = refs[3 * n : 3 * n + 3], refs[3 * n + 3 :]
    new_m, new_v = rest[:n], rest[n:]
    factor = factor_ref[0:1, 0:1]
    first = pl.program_id(0) == 0
    for i, (at, lane) in enumerate(places):
        rows, columns = m[i].shape[1:]
        for c in range(0, columns, 256):
            width = min(256, columns - c)
            here = slice(at + c // 256 * rows, at + c // 256 * rows + rows)
            if at < unit:
                g = jnp.where(first, both[here, lane : lane + width], early[here, lane : lane + width])
            else:
                g = jnp.where(first, late[here.start - unit : here.stop - unit, lane : lane + width], both[here, lane : lane + width])
            g = g.astype(F32) * factor
            across = slice(c, c + width)
            a = 0.9 * m[i][0, :, across] + 0.1 * g
            b = 0.95 * v[i][0, :, across] + 0.05 * g * g
            new_m[i][0, :, across] = a
            new_v[i][0, :, across] = b
            old = w[i][0, :, across].astype(F32)
            fresh[0, here, lane : lane + width] = (old - 0.02 * (a * lax.rsqrt(b + 1e-8) + 0.1 * old)).astype(BF16)


def adamw(weights, m, v, packed, factor, me, places, unit):
    layers = weights[0].shape[0]
    mine = [pl.BlockSpec((1, a.shape[1], a.shape[2]), lambda l, i: (l, i[0], 0)) for a in m]
    own = [pl.BlockSpec((1, a.shape[1], a.shape[2]), lambda l, *_: (l, 0, 0)) for a in m]
    height = packed[0].shape[0] + packed[2].shape[0]
    outs = [jax.ShapeDtypeStruct((layers, height, 256), BF16)] + [jax.ShapeDtypeStruct(a.shape, F32) for a in (*m, *v)]
    return pl.pallas_call(
        functools.partial(_adamw, places=places, unit=unit),
        grid_spec=pltpu.PrefetchScalarGridSpec(
            num_scalar_prefetch=1,
            grid=(layers,),
            in_specs=[pl.BlockSpec(factor.shape, lambda l, *_: (0, 0))] + mine + own + own + [pl.BlockSpec(a.shape, lambda l, *_: (0, 0)) for a in packed],
            out_specs=[pl.BlockSpec((1, height, 256), lambda l, *_: (l, 0, 0))] + own + own,
        ),
        out_shape=outs,
        compiler_params=_params("arbitrary"),
        name="adamw",
    )(me, factor, *weights, *m, *v, *packed)


def _unpack(pack_ref, *outs, places):
    for (at, lane), out in zip(places, outs):
        _, rows, columns = out.shape
        for c in range(0, columns, 256):
            width = min(256, columns - c)
            out[0, :, c : c + width] = pack_ref[0, 0, at + c // 256 * rows : at + c // 256 * rows + rows, lane : lane + width]


def unpack(gathered, m, places):
    group, layers, height, _ = gathered.shape
    return pl.pallas_call(
        functools.partial(_unpack, places=places),
        grid=(layers, group),
        in_specs=[pl.BlockSpec((1, 1, height, 256), lambda l, i: (i, l, 0, 0))],
        out_specs=[pl.BlockSpec((1, a.shape[1], a.shape[2]), lambda l, i: (l, i, 0)) for a in m],
        out_shape=[jax.ShapeDtypeStruct((layers, group * a.shape[1], a.shape[2]), BF16) for a in m],
        compiler_params=_params("arbitrary", "arbitrary"),
        name="unpack",
    )(gathered)


def _meet(peers):
    barrier = pltpu.get_barrier_semaphore()
    for peer in peers:
        pl.semaphore_signal(barrier, inc=1, device_id={"dp": peer}, device_id_type=pl.DeviceIdType.MESH)
    pl.semaphore_wait(barrier, len(peers))


def _send(src, dst, send, recv, peer):
    copy = pltpu.make_async_remote_copy(src_ref=src, dst_ref=dst, send_sem=send, recv_sem=recv, device_id={"dp": peer}, device_id_type=pl.DeviceIdType.MESH)
    copy.start()
    return copy


def _scatter(x_ref, out_ref, near_s, mine_s, far_s, send1, recv1, send2, recv2, *, chips):
    me = lax.axis_index("dp")
    chip, core = lax.div(me, 2), lax.rem(me, 2)
    partner = chip * 2 + 1 - core
    turn = [lax.rem(chip + n, chips) for n in range(chips)]
    _meet([partner] + [c * 2 + core for c in turn[1:]])
    order = [*range(1, chips), 0]
    first = {n: _send(x_ref.at[turn[n] * 2 + 1 - core], near_s.at[n], send1.at[n], recv1.at[n], partner) for n in order}
    second = {}
    for n in order[:-1]:
        first[n].wait_recv()
        mine_s[n] = (x_ref[turn[n] * 2 + core].astype(F32) + near_s[n].astype(F32)).astype(BF16)
        second[n] = _send(mine_s.at[n], far_s.at[n], send2.at[n], recv2.at[n], turn[n] * 2 + core)
    first[0].wait_recv()
    total = x_ref[me].astype(F32) + near_s[0].astype(F32)
    for n in order[:-1]:
        second[n].wait_recv()
        total += far_s[n].astype(F32)
    out_ref[...] = total.astype(BF16)
    for n in order:
        first[n].wait_send()
    for n in order[:-1]:
        second[n].wait_send()


def scatter(x):
    group, rows, width = x.shape
    chips = group // 2
    block = (chips, rows, width)
    vmem = pl.BlockSpec(memory_space=pltpu.VMEM)
    return pl.pallas_call(
        functools.partial(_scatter, chips=chips),
        in_specs=[vmem],
        out_specs=vmem,
        out_shape=jax.ShapeDtypeStruct((rows, width), BF16),
        scratch_shapes=[pltpu.VMEM(block, BF16)] * 3 + [pltpu.SemaphoreType.DMA((chips,))] * 4,
        compiler_params=pltpu.CompilerParams(collective_id=0, has_side_effects=True, vmem_limit_bytes=VMEM),
        cost_estimate=pl.CostEstimate(flops=40_000_000_000, transcendentals=0, bytes_accessed=x.size * 2),
        name="scatter",
    )(x)


def _clip(*refs, group, count):
    *blocks, out_ref, part_s, all_s, send, recv = refs
    me = lax.axis_index("dp")
    peers = [lax.rem(me + n, group) for n in range(1, group)]
    part = sum(jnp.sum(jnp.square(b[...].astype(F32)), axis=0, keepdims=True) for b in blocks)
    part_s[...] = jnp.broadcast_to(part[:, :128] + part[:, 128:], part_s.shape)
    _meet(peers)
    copies = [_send(part_s, all_s.at[me], send.at[n], recv.at[n], peer) for n, peer in enumerate(peers)]
    all_s[me] = part_s[...]
    for copy in copies:
        copy.wait_recv()
    total = jnp.sum(jnp.sum(all_s[...], axis=0), axis=1, keepdims=True)
    out_ref[...] = jnp.broadcast_to(jnp.minimum(1.0, 0.5 * lax.rsqrt(total / count + 1e-30)), out_ref.shape)
    for copy in copies:
        copy.wait_send()


def clip(blocks, group, count):
    vmem = pl.BlockSpec(memory_space=pltpu.VMEM)
    return pl.pallas_call(
        functools.partial(_clip, group=group, count=count),
        in_specs=[vmem] * len(blocks),
        out_specs=vmem,
        out_shape=jax.ShapeDtypeStruct((8, 128), F32),
        scratch_shapes=[pltpu.VMEM((8, 128), F32), pltpu.VMEM((group, 8, 128), F32)] + [pltpu.SemaphoreType.DMA((group - 1,))] * 2,
        compiler_params=pltpu.CompilerParams(collective_id=1, has_side_effects=True, vmem_limit_bytes=VMEM),
        name="clip",
    )(*blocks)


def angles(tokens):
    half = HEAD // 2
    angle = jnp.arange(tokens, dtype=F32)[:, None] * THETA ** (-jnp.arange(half, dtype=F32) / half)
    cos, sin = jnp.cos(angle), jnp.sin(angle)
    return jnp.concatenate([cos, cos], -1), jnp.concatenate([-sin, sin], -1)


def layout(m):
    q, k, v, o, gate, up, down = (a.shape[1] * a.shape[2] // 256 for a in m)
    unit = gate + up + down
    rest = q + k + v + o
    block = min(n for n in range(16, unit + 1, 16) if n >= rest and unit % n == 0)
    places = ((unit, 0), (unit + q, 0), (unit + q, m[1].shape[2]), (unit + q + k + v, 0), (0, 0), (gate, 0), (gate + up, 0))
    return places, unit, rest, unit + block


def solution(mesh):
    group = mesh.shape["dp"]

    def step(x, dy, *arrays):
        weights, m, v = (arrays[i : i + 7] for i in (0, 7, 14))
        wq, wk, wv, wo, wg, wu, wd = weights
        layers = wq.shape[0]
        places, unit, rest, pack = layout(m)
        cos, sin = angles(x.shape[1])
        h, kept = x[0], []
        for n in range(layers):
            q, k, val = project(h, wq, wk, wv, cos, sin, n)
            o, lse = attend(q, k, val)
            mid, out = feed(o, h, wo, wg, wu, wd, n)
            kept.append((h, q, k, val, o, lse, mid))
            h = out
        summed = lambda a: lax.psum_scatter(a, "dp", scatter_dimension=0, tiled=True)[0]

        def unit_bwd(n, by_h, packed=None):
            return feed_bwd(kept[n][6], by_h, wg, wu, wd, n, group, packed)

        def rest_bwd(n, dmid, at, height):
            h, q, k, val, o, lse, _ = kept[n]
            do, delta = out_bwd(dmid, o, wo, n)
            dq, dk, dv = attend_bwd(q, k, val, do, lse, delta)
            return project_bwd(dq, dk, dv, h, dmid, o, wq, wk, wv, cos, sin, n, group, at, height)

        early, dmid = unit_bwd(1, dy[0])
        early = summed(early)
        both, by_h = rest_bwd(1, dmid, unit, pack)
        both, dmid = unit_bwd(0, by_h, both)
        both = summed(both)
        late, _ = rest_bwd(0, dmid, 0, rest)
        mine = [early, both, scatter(late)]
        factor = clip(mine, group, sum(w.size for w in weights))
        me = lax.axis_index("dp").astype(jnp.int32)
        fresh, *moments = adamw(weights, m, v, mine, factor, me.reshape(1), places, unit)
        whole = unpack(lax.all_gather(fresh, "dp", axis=0), m, places)
        return (*whole, *moments)

    states, all_of, cut = P(("rep", "dp"), None, None), P(None, None, None), P(None, "dp", None)
    return jax.shard_map(
        step,
        mesh=mesh,
        in_specs=(states, states) + (all_of,) * 7 + (cut,) * 14,
        out_specs=(P("rep", None, None),) * 7 + (P("rep", "dp", None),) * 14,
        check_vma=False,
    )
```

```python
import functools

import jax
import numpy as np
import jax.numpy as jnp
from jax import lax
from jax.experimental import pallas as pl
from jax.experimental.pallas import tpu as pltpu
from jax.sharding import PartitionSpec as P

NEG = -1e30
HIDDEN = 2 * NEG
LOG2E = 1.4426950408889634
VMEM = 62 * 2**20
HEAD = 128
THETA = 10000
EPS = 1e-6
F32, BF16 = jnp.float32, jnp.bfloat16


def _dot(a, b, ca, cb):
    return lax.dot_general(a, b, (((ca,), (cb,)), ((), ())), preferred_element_type=F32)


def _params(*semantics):
    return pltpu.CompilerParams(dimension_semantics=semantics, vmem_limit_bytes=VMEM)


def _cost(flops, arrays, exps=0):
    return pl.CostEstimate(flops=int(flops), transcendentals=int(exps), bytes_accessed=sum(a.size * a.dtype.itemsize for a in arrays))


def _rows(n):
    return slice(n * HEAD, (n + 1) * HEAD)


def _scale(wide):
    return lax.rsqrt(jnp.mean(wide * wide, -1, keepdims=True) + EPS)


def _normed(h):
    wide = h.astype(F32)
    return (wide * _scale(wide)).astype(BF16)


def _norm_bwd(h, ct):
    wide, c = h.astype(F32), ct.astype(BF16).astype(F32)
    scale = _scale(wide)
    back = jnp.mean(c * wide, -1, keepdims=True) * (scale * scale * scale)
    return (c * scale - wide * back).astype(BF16)


def _turn(t, cos, sin):
    t = t.astype(F32)
    return (t * cos + pltpu.roll(t, HEAD // 2, 1) * sin).astype(BF16)


def _turn_back(t, cos, sin):
    t = t.astype(F32)
    return (t * cos - pltpu.roll(t, HEAD // 2, 1) * sin).astype(BF16)


def _whole(shape, layer=None):
    if layer is None:
        return pl.BlockSpec(shape, lambda *_: (0,) * len(shape), pipeline_mode=pl.Buffered(1))
    return pl.BlockSpec((1, *shape), lambda *_: (layer,) + (0,) * len(shape), pipeline_mode=pl.Buffered(1))


def _pack(ref, at, value, height):
    for c in range(value.shape[1] // 256):
        piece = value[:, c * 256 : (c + 1) * 256].astype(BF16)
        ref[:, at + c * height : at + (c + 1) * height, :] = piece.reshape(-1, height, 256)


def _project(h_ref, wq_ref, wk_ref, wv_ref, cos_ref, sin_ref, q_ref, k_ref, v_ref):
    a = _normed(h_ref[...])
    cos, sin = cos_ref[...], sin_ref[...]
    q = _dot(a, wq_ref[0], 1, 0).astype(BF16)
    for n in range(q.shape[1] // HEAD):
        q_ref[:, _rows(n)] = _turn(q[:, _rows(n)], cos, sin)
    k_ref[...] = _turn(_dot(a, wk_ref[0], 1, 0).astype(BF16), cos, sin)
    v_ref[...] = _dot(a, wv_ref[0], 1, 0).astype(BF16)


def project(h, wq, wk, wv, cos, sin, layer, bt=512):
    t, d = h.shape
    tokens = lambda width: pl.BlockSpec((bt, width), lambda i: (i, 0))
    wide, one = wq.shape[2], wk.shape[2]
    outs = [jax.ShapeDtypeStruct((t, w), BF16) for w in (wide, one, one)]
    return pl.pallas_call(
        _project,
        grid=(t // bt,),
        in_specs=[tokens(d), _whole((d, wide), layer), _whole((d, one), layer), _whole((d, one), layer), tokens(HEAD), tokens(HEAD)],
        out_specs=[tokens(wide), tokens(one), tokens(one)],
        out_shape=outs,
        compiler_params=_params("arbitrary"),
        cost_estimate=_cost(2 * t * d * (wide + 2 * one), [h, cos, sin, *outs]),
        name="project",
    )(h, wq, wk, wv, cos, sin)


def _attend(q_ref, k_ref, v_ref, o_ref, lse_ref, top_s, mix_s, gap_s, *, heads, bq, scale):
    iq = pl.program_id(0)
    e = scale * LOG2E
    cols = [slice(n * bq, (n + 1) * bq) for n in range(heads)]

    half = bq // 2

    @pl.when(iq == 0)
    def _():
        gap_s[...] = lax.broadcasted_iota(jnp.int32, (half, bq), 1) - lax.broadcasted_iota(jnp.int32, (half, bq), 0)

    top_s[...] = jnp.full(top_s.shape, NEG, F32)
    mix_s[...] = jnp.zeros(mix_s.shape, F32)

    def block(start, size, lo, masked):
        here = pl.ds(pl.multiple_of(start, size), size)
        key = k_ref[here, :]
        scores = [_dot(key, q_ref[lo:, _rows(n)], 1, 1) for n in range(heads)]
        ok = gap_s[:, : bq - lo] >= 0 if masked else None
        weights, keeps = [], []
        for n, s in enumerate(scores):
            if masked:
                s = jnp.where(ok, s, HIDDEN)
            at = slice(n * bq + lo, (n + 1) * bq)
            old = top_s[:, at]
            top = jnp.maximum(old, s.max(axis=0, keepdims=True))
            top_s[:, at] = top
            weights.append(jnp.exp2((s - top) * e).astype(BF16))
            keeps.append(jnp.exp2((old - top) * e))
        values = jnp.concatenate([v_ref[here, :].T, jnp.ones((8, size), BF16)], axis=0)
        for n, (p, keep) in enumerate(zip(weights, keeps)):
            at = slice(n * bq + lo, (n + 1) * bq)
            mix_s[:, at] = mix_s[:, at] * keep + _dot(values, p, 1, 0)

    lax.fori_loop(0, iq, lambda j, _: block(j * bq, bq, 0, False), None)
    block(iq * bq, half, 0, True)
    block(iq * bq + half, half, half, True)
    for n in range(heads):
        total = mix_s[HEAD : HEAD + 1, cols[n]]
        o_ref[:, _rows(n)] = (mix_s[:HEAD, cols[n]] * (1 / total)).T.astype(BF16)
        lse_ref[n : n + 1, :] = top_s[:, cols[n]] * scale + jnp.log(total)


def attend(q, k, v, bq=512):
    t, wide = q.shape
    heads = wide // HEAD
    outs = [jax.ShapeDtypeStruct((t, wide), BF16), jax.ShapeDtypeStruct((heads, t), F32)]
    return pl.pallas_call(
        functools.partial(_attend, heads=heads, bq=bq, scale=HEAD**-0.5),
        grid=(t // bq,),
        in_specs=[pl.BlockSpec((bq, wide), lambda i: (i, 0)), _whole((t, HEAD)), _whole((t, HEAD))],
        out_specs=[pl.BlockSpec((bq, wide), lambda i: (i, 0)), pl.BlockSpec((heads, bq), lambda i: (0, i))],
        out_shape=outs,
        scratch_shapes=[pltpu.VMEM((1, heads * bq), F32), pltpu.VMEM((HEAD + 8, heads * bq), F32), pltpu.VMEM((bq // 2, bq), jnp.int32)],
        compiler_params=_params("arbitrary"),
        cost_estimate=_cost(4 * t * t * wide, [q, k, v, *outs], heads * t * t),
        name="attend",
    )(q, k, v)


def _feed(o_ref, h_ref, wo_ref, wg_ref, wu_ref, wd_ref, mid_ref, out_ref, *, bf):
    mid = h_ref[...] + _dot(o_ref[...], wo_ref[0], 1, 0).astype(BF16)
    mid_ref[...] = mid
    b = _normed(mid)
    total = None
    for at in range(0, wg_ref.shape[2], bf):
        gate = _dot(b, wg_ref[0, :, at : at + bf], 1, 0)
        up = _dot(b, wu_ref[0, :, at : at + bf], 1, 0)
        act = (gate * jax.nn.sigmoid(gate) * up).astype(BF16)
        term = _dot(act, wd_ref[0, at : at + bf, :], 1, 0)
        total = term if total is None else total + term
    out_ref[...] = mid + total.astype(BF16)


def feed(o, h, wo, wg, wu, wd, layer, bt=512, bf=512):
    t, d = h.shape
    ff = wg.shape[2]
    tokens = lambda width: pl.BlockSpec((bt, width), lambda i: (i, 0))
    outs = [jax.ShapeDtypeStruct((t, d), BF16)] * 2
    return pl.pallas_call(
        functools.partial(_feed, bf=bf),
        grid=(t // bt,),
        in_specs=[tokens(o.shape[1]), tokens(d), _whole(wo.shape[1:], layer), _whole((d, ff), layer), _whole((d, ff), layer), _whole((ff, d), layer)],
        out_specs=[tokens(d), tokens(d)],
        out_shape=outs,
        compiler_params=_params("arbitrary"),
        cost_estimate=_cost(2 * t * d * (o.shape[1] + 3 * ff), [o, h, *outs], t * ff),
        name="feed",
    )(o, h, wo, wg, wu, wd)


def _feed_bwd(mid_ref, dy_ref, wg_ref, wu_ref, wd_ref, *rest, bt, own, down, steps, first):
    pack_ref, dmid_ref, pack_s, b_s, bt_s, dyt_s, db_s, dg_s, act_s, sems = rest[-10:]
    j = pl.program_id(0)
    t, bf = mid_ref.shape[0], wg_ref.shape[2]

    def copies(step):
        places = [(slice(None), pl.ds((half * steps + step) * own, own), pl.ds(first + (half * steps + step) * own, own)) for half in range(2)]
        high = pack_s.shape[1] - 2 * steps * own
        places.append((pl.ds(step * (bf // down), bf // down), pl.ds(2 * steps * own, high), pl.ds(first + 2 * steps * own, high)))
        return [pltpu.make_async_copy(pack_s.at[who, here, :], pack_ref.at[who, there, :], sems.at[step, n]) for n, (who, here, there) in enumerate(places)]

    blocks = [slice(at, at + bt) for at in range(0, t, bt)]

    @pl.when(j == 0)
    def _():
        for at in blocks:
            b = _normed(mid_ref[at, :])
            b_s[at, :] = b
            bt_s[:, at] = b.T
            dyt_s[:, at] = dy_ref[at, :].T
            db_s[at, :] = jnp.zeros((bt, db_s.shape[1]), F32)

    w_gate, w_up, w_down = wg_ref[0], wu_ref[0], wd_ref[0]
    both = jnp.concatenate([w_gate, w_up], axis=1)
    for at in blocks:
        b = b_s[at, :]
        gate = _dot(b, w_gate, 1, 0)
        up = _dot(b, w_up, 1, 0)
        dact = _dot(dy_ref[at, :], w_down, 1, 1).astype(BF16).astype(F32)
        s = jax.nn.sigmoid(gate)
        silu = gate * s
        act_s[at, :] = (silu * up).astype(BF16)
        dup = (dact * silu).astype(BF16)
        dgate = (dact * up * (s + silu * (1 - s))).astype(BF16)
        dg_s[at, :bf] = dgate
        dg_s[at, bf:] = dup
        db_s[at, :] += _dot(dg_s[at, :], both, 1, 1)
    @pl.when(j > 0)
    def _():
        for copy in copies(j - 1):
            copy.start()

    by_in = _dot(bt_s[...], dg_s[...], 1, 0).astype(BF16)
    for half in range(2):
        at = pl.multiple_of((half * steps + j) * own, own)
        pack_s[:, pl.ds(at, own), :] = by_in[:, half * bf : (half + 1) * bf].reshape(-1, own, bf)
    by_down = _dot(dyt_s[...], act_s[...], 1, 0).T.astype(BF16)
    for i in range(bf // down):
        for c in range(by_down.shape[1] // bf):
            at = 2 * steps * own + c * down
            pack_s[j * (bf // down) + i, at : at + down, :] = by_down[i * down : (i + 1) * down, c * bf : (c + 1) * bf]

    @pl.when(j == steps - 1)
    def _():
        for at in blocks:
            dmid_ref[at, :] = dy_ref[at, :] + _norm_bwd(mid_ref[at, :], db_s[at, :])
        for copy in copies(j):
            copy.start()
        for step in range(steps):
            for copy in copies(step):
                copy.wait()


def feed_bwd(mid, dy, wg, wu, wd, layer, group, packed=None, bt=512, bf=256):
    t, d = mid.shape
    ff = wg.shape[2]
    own, down = d // group, ff // group
    rows = (2 * own * ff + down * d) // 256
    height = rows if packed is None else packed.shape[1]
    more = [] if packed is None else [packed]
    outs = [jax.ShapeDtypeStruct((group, height, 256), BF16), jax.ShapeDtypeStruct((t, d), BF16)]
    return pl.pallas_call(
        functools.partial(_feed_bwd, bt=bt, own=own, down=down, steps=ff // bf, first=height - rows),
        grid=(ff // bf,),
        in_specs=[_whole((t, d)), _whole((t, d)), pl.BlockSpec((1, d, bf), lambda j: (layer, 0, j)), pl.BlockSpec((1, d, bf), lambda j: (layer, 0, j)),
                  pl.BlockSpec((1, bf, d), lambda j: (layer, j, 0))] + [pl.BlockSpec(memory_space=pl.ANY)] * len(more),
        input_output_aliases={5: 0} if more else {},
        out_specs=[pl.BlockSpec(memory_space=pl.ANY), _whole((t, d))],
        out_shape=outs,
        scratch_shapes=[pltpu.VMEM((group, rows, 256), BF16), pltpu.VMEM((t, d), BF16), pltpu.VMEM((d, t), BF16), pltpu.VMEM((d, t), BF16),
                        pltpu.VMEM((t, d), F32), pltpu.VMEM((t, 2 * bf), BF16), pltpu.VMEM((t, bf), BF16), pltpu.SemaphoreType.DMA((ff // bf, 3))],
        compiler_params=_params("arbitrary"),
        cost_estimate=_cost(16 * t * d * ff, [mid, dy, *outs], t * ff),
        name="feed_bwd",
    )(mid, dy, wg, wu, wd, *more)


def _attend_bwd(q_ref, k_ref, v_ref, dmid_ref, o_ref, lse_ref, wo_ref, dq_ref, dk_ref, dv_ref, dq_s, dk_s, dv_s, do_s, stat_s, gap_s,
                *, heads, bq, pair, scale):
    iq = pl.program_id(0)
    e = scale * LOG2E
    wide = pair * bq
    groups = [range(n, n + pair) for n in range(0, heads, pair)]

    @pl.when(iq == 0)
    def _():
        gap_s[...] = lax.rem(lax.broadcasted_iota(jnp.int32, (bq, wide), 1), bq) - lax.broadcasted_iota(jnp.int32, (bq, wide), 0)
        dk_s[...] = jnp.zeros_like(dk_s)
        dv_s[...] = jnp.zeros_like(dv_s)

    dq_s[...] = jnp.zeros_like(dq_s)
    do = _dot(dmid_ref[...], wo_ref[0], 1, 1).astype(BF16)
    for n in range(heads):
        at = slice(n * bq, (n + 1) * bq)
        do_s[at, :] = do[:, _rows(n)]
        stat_s[0:1, at] = lse_ref[n : n + 1, :] * LOG2E
        stat_s[1:2, at] = (do[:, _rows(n)].astype(F32) * o_ref[:, _rows(n)].astype(F32)).T.sum(axis=0, keepdims=True)

    def block(start, size, masked):
        here = pl.ds(pl.multiple_of(start, bq), size)
        key, value = k_ref[here, :], v_ref[here, :]
        qs = [jnp.concatenate([q_ref[:, _rows(n)] for n in g], axis=0) for g in groups]
        dos = [do_s[i * wide : (i + 1) * wide, :] for i in range(len(groups))]
        scores = [_dot(key, x, 1, 1) for x in qs]
        dps = [_dot(value, x, 1, 1) for x in dos]
        ok = gap_s[...] >= 0 if masked else None
        for i in range(len(groups)):
            at = slice(i * wide, (i + 1) * wide)
            p = jnp.exp2(scores[i] * e - stat_s[0:1, at])
            if masked:
                p = jnp.where(ok, p, 0.0)
            ds = (p * (dps[i] - stat_s[1:2, at])).astype(BF16)
            dv_s[here, :] += _dot(p.astype(BF16), dos[i], 1, 0)
            dk_s[here, :] += _dot(ds, qs[i], 1, 0)
            dq_s[:, at] += _dot(key.T, ds, 1, 0)

    pairs = lax.div(iq, 2)
    lax.fori_loop(0, pairs, lambda j, _: block(j * 2 * bq, 2 * bq, False), None)
    pl.when(lax.rem(iq, 2) == 1)(lambda: block((iq - 1) * bq, bq, False))
    block(iq * bq, bq, True)
    for n in range(heads):
        dq_ref[:, _rows(n)] = (dq_s[:, n * bq : (n + 1) * bq] * scale).T.astype(BF16)

    @pl.when(iq == pl.num_programs(0) - 1)
    def _():
        dk_ref[...] = (dk_s[...] * scale).astype(BF16)
        dv_ref[...] = dv_s[...].astype(BF16)


def attend_bwd(q, k, v, dmid, o, lse, wo, layer, bq=256, pair=1):
    t, wide = q.shape
    heads, d = wide // HEAD, dmid.shape[1]
    outs = [jax.ShapeDtypeStruct((t, wide), BF16)] + [jax.ShapeDtypeStruct((t, HEAD), BF16)] * 2
    queries, states, stats = pl.BlockSpec((bq, wide), lambda i: (i, 0)), pl.BlockSpec((bq, d), lambda i: (i, 0)), pl.BlockSpec((heads, bq), lambda i: (0, i))
    return pl.pallas_call(
        functools.partial(_attend_bwd, heads=heads, bq=bq, pair=pair, scale=HEAD**-0.5),
        grid=(t // bq,),
        in_specs=[queries, _whole((t, HEAD)), _whole((t, HEAD)), states, queries, stats, _whole((wide, d), layer)],
        out_specs=[queries, _whole((t, HEAD)), _whole((t, HEAD))],
        out_shape=outs,
        scratch_shapes=[pltpu.VMEM((HEAD, heads * bq), F32), pltpu.VMEM((t, HEAD), F32), pltpu.VMEM((t, HEAD), F32),
                        pltpu.VMEM((heads * bq, HEAD), BF16), pltpu.VMEM((2, heads * bq), F32), pltpu.VMEM((bq, pair * bq), jnp.int32)],
        compiler_params=_params("arbitrary"),
        cost_estimate=_cost(10 * t * t * wide, [q, k, v, dmid, o, *outs], heads * t * t),
        name="attend_bwd",
    )(q, k, v, dmid, o, lse, wo)


def _project_bwd(dq_ref, dk_ref, dv_ref, h_ref, dmid_ref, o_ref, wq_ref, wk_ref, wv_ref, cos_ref, sin_ref, pack_ref, dh_ref, qkv_s, o_s, *, own):
    i = pl.program_id(0)
    cos, sin = cos_ref[...], sin_ref[...]
    wide = dq_ref.shape[1]
    dq = jnp.concatenate([_turn_back(dq_ref[:, _rows(n)], cos, sin) for n in range(wide // HEAD)], axis=1)
    dkv = jnp.concatenate([_turn_back(dk_ref[...], cos, sin), dv_ref[...]], axis=1)
    h, dmid = h_ref[...], dmid_ref[...]
    by_a = _dot(dq, wq_ref[0], 1, 1) + _dot(dkv, jnp.concatenate([wk_ref[0], wv_ref[0]], axis=1), 1, 1)
    dh_ref[...] = dmid + _norm_bwd(h, by_a)
    a = _normed(h).T
    by_q, by_kv, by_o = _dot(a, dq, 1, 0), _dot(a, dkv, 1, 0), _dot(o_ref[...].T, dmid, 1, 0)

    @pl.when(i == 0)
    def _():
        qkv_s[:, :wide] = by_q
        qkv_s[:, wide:] = by_kv
        o_s[...] = by_o

    @pl.when(i > 0)
    def _():
        qkv_s[:, :wide] += by_q
        qkv_s[:, wide:] += by_kv
        o_s[...] += by_o

    @pl.when(i == pl.num_programs(0) - 1)
    def _():
        _pack(pack_ref, 0, qkv_s[...], own)
        used = qkv_s.shape[1] // 256 * own
        high = o_s.shape[0] // pack_ref.shape[0]
        _pack(pack_ref, used, o_s[...], high)


def project_bwd(dq, dk, dv, h, dmid, o, wq, wk, wv, cos, sin, layer, group, rows, pack, bt=512):
    t, d = h.shape
    wide, one = dq.shape[1], dk.shape[1]
    tokens = lambda width: pl.BlockSpec((bt, width), lambda i: (i, 0))
    outs = [jax.ShapeDtypeStruct((group, pack, 256), BF16), jax.ShapeDtypeStruct((t, d), BF16)]
    return pl.pallas_call(
        functools.partial(_project_bwd, own=d // group),
        grid=(t // bt,),
        in_specs=[tokens(wide), tokens(one), tokens(one), tokens(d), tokens(d), tokens(wide), _whole((d, wide), layer), _whole((d, one), layer),
                  _whole((d, one), layer), tokens(HEAD), tokens(HEAD)],
        out_specs=[pl.BlockSpec((group, rows, 256), lambda i: (0, 0, 0)), tokens(d)],
        out_shape=outs,
        scratch_shapes=[pltpu.VMEM((d, wide + 2 * one), F32), pltpu.VMEM((wide, d), F32)],
        compiler_params=_params("arbitrary"),
        cost_estimate=_cost(4 * t * d * (2 * wide + 2 * one), [dq, h, dmid, o, outs[1]]),
        name="project_bwd",
    )(dq, dk, dv, h, dmid, o, wq, wk, wv, cos, sin)


def _adamw(me_ref, factor_ref, *refs, places, rest):
    n = len(places)
    w, m, v = refs[:n], refs[n : 2 * n], refs[2 * n : 3 * n]
    (early, both, late), (fresh, *moments) = refs[3 * n : 3 * n + 3], refs[3 * n + 3 :]
    new_m, new_v = moments[:n], moments[n:]
    factor = factor_ref[0:1, 0:1]
    first = pl.program_id(0) == 0
    for i, (at, lane) in enumerate(places):
        rows, columns = m[i].shape[1:]
        for c in range(0, columns, 256):
            width = min(256, columns - c)
            here = slice(at + c // 256 * rows, at + c // 256 * rows + rows)
            if at < rest:
                g = jnp.where(first, late[here, lane : lane + width], both[here, lane : lane + width])
            else:
                g = jnp.where(first, both[here, lane : lane + width], early[here.start - rest : here.stop - rest, lane : lane + width])
            g = g.astype(F32) * factor
            across = slice(c, c + width)
            a = 0.9 * m[i][0, :, across] + 0.1 * g
            b = 0.95 * v[i][0, :, across] + 0.05 * g * g
            new_m[i][0, :, across] = a
            new_v[i][0, :, across] = b
            old = w[i][0, :, across].astype(F32)
            fresh[0, here, lane : lane + width] = (old - 0.02 * (a * lax.rsqrt(b + 1e-8) + 0.1 * old)).astype(BF16)


def adamw(weights, m, v, packed, factor, me, places, rest):
    layers = weights[0].shape[0]
    mine = [pl.BlockSpec((1, a.shape[1], a.shape[2]), lambda l, i: (l, i[0], 0)) for a in m]
    own = [pl.BlockSpec((1, a.shape[1], a.shape[2]), lambda l, *_: (l, 0, 0)) for a in m]
    height = packed[0].shape[0] + packed[2].shape[0]
    outs = [jax.ShapeDtypeStruct((layers, height, 256), BF16)] + [jax.ShapeDtypeStruct(a.shape, F32) for a in (*m, *v)]
    return pl.pallas_call(
        functools.partial(_adamw, places=places, rest=rest),
        grid_spec=pltpu.PrefetchScalarGridSpec(
            num_scalar_prefetch=1,
            grid=(layers,),
            in_specs=[pl.BlockSpec(factor.shape, lambda l, *_: (0, 0))] + mine + own + own + [pl.BlockSpec(a.shape, lambda l, *_: (0, 0)) for a in packed],
            out_specs=[pl.BlockSpec((1, height, 256), lambda l, *_: (l, 0, 0))] + own + own,
        ),
        out_shape=outs,
        compiler_params=_params("arbitrary"),
        name="adamw",
    )(me, factor, *weights, *m, *v, *packed)


def _unpack(pack_ref, *outs, places):
    for (at, lane), out in zip(places, outs):
        rows = out.shape[1] // pack_ref.shape[0]
        for i in range(pack_ref.shape[0]):
            for c in range(0, out.shape[2], 256):
                width = min(256, out.shape[2] - c)
                first = at + c // 256 * rows
                out[:, i * rows : (i + 1) * rows, c : c + width] = pack_ref[i, :, first : first + rows, lane : lane + width]


def unpack(gathered, m, places, some=4):
    group, layers, height, _ = gathered.shape
    return pl.pallas_call(
        functools.partial(_unpack, places=places),
        grid=(group // some,),
        in_specs=[pl.BlockSpec((some, layers, height, 256), lambda i: (i, 0, 0, 0))],
        out_specs=[pl.BlockSpec((layers, some * a.shape[1], a.shape[2]), lambda i: (0, i, 0)) for a in m],
        out_shape=[jax.ShapeDtypeStruct((layers, group * a.shape[1], a.shape[2]), BF16) for a in m],
        compiler_params=_params("arbitrary"),
        name="unpack",
    )(gathered)


def _meet(peers):
    barrier = pltpu.get_barrier_semaphore()
    for peer in peers:
        pl.semaphore_signal(barrier, inc=1, device_id={"dp": peer}, device_id_type=pl.DeviceIdType.MESH)
    pl.semaphore_wait(barrier, len(peers))


def _send(src, dst, send, recv, peer):
    copy = pltpu.make_async_remote_copy(src_ref=src, dst_ref=dst, send_sem=send, recv_sem=recv, device_id={"dp": peer}, device_id_type=pl.DeviceIdType.MESH)
    copy.start()
    return copy


def _scatter(x_ref, out_ref, near_s, mine_s, far_s, send1, recv1, send2, recv2, *, chips):
    me = lax.axis_index("dp")
    chip, core = lax.div(me, 2), lax.rem(me, 2)
    partner = chip * 2 + 1 - core
    turn = [lax.rem(chip + n, chips) for n in range(chips)]
    _meet([partner] + [c * 2 + core for c in turn[1:]])
    order = [*range(1, chips), 0]
    first = {n: _send(x_ref.at[turn[n] * 2 + 1 - core], near_s.at[n], send1.at[n], recv1.at[n], partner) for n in order}
    second = {}
    for n in order[:-1]:
        first[n].wait_recv()
        mine_s[n] = (x_ref[turn[n] * 2 + core].astype(F32) + near_s[n].astype(F32)).astype(BF16)
        second[n] = _send(mine_s.at[n], far_s.at[n], send2.at[n], recv2.at[n], turn[n] * 2 + core)
    first[0].wait_recv()
    total = x_ref[me].astype(F32) + near_s[0].astype(F32)
    for n in order[:-1]:
        second[n].wait_recv()
        total += far_s[n].astype(F32)
    out_ref[...] = total.astype(BF16)
    for n in order:
        first[n].wait_send()
    for n in order[:-1]:
        second[n].wait_send()


def scatter(x):
    group, rows, width = x.shape
    chips = group // 2
    block = (chips, rows, width)
    vmem = pl.BlockSpec(memory_space=pltpu.VMEM)
    return pl.pallas_call(
        functools.partial(_scatter, chips=chips),
        in_specs=[vmem],
        out_specs=vmem,
        out_shape=jax.ShapeDtypeStruct((rows, width), BF16),
        scratch_shapes=[pltpu.VMEM(block, BF16)] * 3 + [pltpu.SemaphoreType.DMA((chips,))] * 4,
        compiler_params=pltpu.CompilerParams(collective_id=0, has_side_effects=True, vmem_limit_bytes=VMEM),
        cost_estimate=pl.CostEstimate(flops=40_000_000_000, transcendentals=0, bytes_accessed=x.size * 2),
        name="scatter",
    )(x)


def _clip(*refs, group, count):
    *blocks, out_ref, part_s, all_s, send, recv = refs
    me = lax.axis_index("dp")
    peers = [lax.rem(me + n, group) for n in range(1, group)]
    part = sum(jnp.sum(jnp.square(b[...].astype(F32)), axis=0, keepdims=True) for b in blocks)
    part_s[...] = jnp.broadcast_to(part[:, :128] + part[:, 128:], part_s.shape)
    _meet(peers)
    copies = [_send(part_s, all_s.at[me], send.at[n], recv.at[n], peer) for n, peer in enumerate(peers)]
    all_s[me] = part_s[...]
    for copy in copies:
        copy.wait_recv()
    total = jnp.sum(jnp.sum(all_s[...], axis=0), axis=1, keepdims=True)
    out_ref[...] = jnp.broadcast_to(jnp.minimum(1.0, 0.5 * lax.rsqrt(total / count + 1e-30)), out_ref.shape)
    for copy in copies:
        copy.wait_send()


def clip(blocks, group, count):
    vmem = pl.BlockSpec(memory_space=pltpu.VMEM)
    return pl.pallas_call(
        functools.partial(_clip, group=group, count=count),
        in_specs=[vmem] * len(blocks),
        out_specs=vmem,
        out_shape=jax.ShapeDtypeStruct((8, 128), F32),
        scratch_shapes=[pltpu.VMEM((8, 128), F32), pltpu.VMEM((group, 8, 128), F32)] + [pltpu.SemaphoreType.DMA((group - 1,))] * 2,
        compiler_params=pltpu.CompilerParams(collective_id=1, has_side_effects=True, vmem_limit_bytes=VMEM),
        name="clip",
    )(*blocks)


def angles(tokens):
    half = HEAD // 2
    turns = np.float32(THETA) ** (-np.arange(half, dtype=np.float32) / np.float32(half))
    angle = (np.arange(tokens, dtype=np.float32)[:, None] * turns.astype(np.float32)).astype(np.float64)
    cos, sin = np.cos(angle).astype(np.float32), np.sin(angle).astype(np.float32)
    return jnp.asarray(np.concatenate([cos, cos], -1)), jnp.asarray(np.concatenate([-sin, sin], -1))


def layout(m):
    q, k, v, o, gate, up, down = (a.shape[1] * a.shape[2] // 256 for a in m)
    rest = q + k + v + o
    places = ((0, 0), (q, 0), (q, m[1].shape[2]), (q + k + v, 0), (rest, 0), (rest + gate, 0), (rest + gate + up, 0))
    return places, rest, rest + gate + up + down


def solution(mesh):
    group = mesh.shape["dp"]

    def step(x, dy, *arrays):
        weights, m, v = (arrays[i : i + 7] for i in (0, 7, 14))
        wq, wk, wv, wo, wg, wu, wd = weights
        layers = wq.shape[0]
        places, rest, pack = layout(m)
        cos, sin = angles(x.shape[1])
        h, kept = x[0], []
        for n in range(layers):
            q, k, val = project(h, wq, wk, wv, cos, sin, n)
            o, lse = attend(q, k, val)
            mid, out = feed(o, h, wo, wg, wu, wd, n)
            kept.append((h, q, k, val, o, lse, mid))
            h = out
        summed = lambda a: lax.psum_scatter(a, "dp", scatter_dimension=0, tiled=True)[0]

        def unit_bwd(n, by_h, packed=None):
            return feed_bwd(kept[n][6], by_h, wg, wu, wd, n, group, packed)

        def rest_bwd(n, dmid, height):
            h, q, k, val, o, lse, _ = kept[n]
            dq, dk, dv = attend_bwd(q, k, val, dmid, o, lse, wo, n)
            return project_bwd(dq, dk, dv, h, dmid, o, wq, wk, wv, cos, sin, n, group, rest, height)

        early, dmid = unit_bwd(1, dy[0])
        early = summed(early)
        both, by_h = rest_bwd(1, dmid, pack)
        both, dmid = unit_bwd(0, by_h, both)
        both = summed(both)
        late, _ = rest_bwd(0, dmid, rest)
        mine = [early, both, scatter(late)]
        factor = clip(mine, group, sum(w.size for w in weights))
        me = lax.axis_index("dp").astype(jnp.int32)
        fresh, *moments = adamw(weights, m, v, mine, factor, me.reshape(1), places, rest)
        whole = unpack(lax.all_gather(fresh, "dp", axis=0), m, places)
        return (*whole, *moments)

    states, all_of, cut = P(("rep", "dp"), None, None), P(None, None, None), P(None, "dp", None)
    return jax.shard_map(
        step,
        mesh=mesh,
        in_specs=(states, states) + (all_of,) * 7 + (cut,) * 14,
        out_specs=(P("rep", None, None),) * 7 + (P("rep", "dp", None),) * 14,
        check_vma=False,
    )
```
